32 devices in a mesh: clip: 2 (over y), outer: 4 (over z), inner: 2 (over x), head: 2 (over core).
Axes of the slice: x: 2, y: 2, z: 4, core: 2. Of those that a mesh axis runs over, the one named last changes fastest.
Arguments:
- tokens: bfloat16 [2, 4096, 3072], P('clip', ('outer', 'inner', 'head')), parts along dimension 0, may hold values from -6 to 6
- shift_mod: float32 [2, 3072], P('clip'), parts along dimension 0, may hold values from -3 to 3
- scale_mod: float32 [2, 3072], P('clip'), parts along dimension 0, may hold values from -1.5 to 1.5
- gate_mod: float32 [2, 3072], P('clip'), parts along dimension 0, may hold values from 0.5 to 2
- query_weight: bfloat16 [3072, 3072], P('outer', ('inner', 'head')), may hold values from -0.109375 to 0.109375
- key_weight: bfloat16 [3072, 3072], P('outer', ('inner', 'head')), may hold values from -0.109375 to 0.109375
- value_weight: bfloat16 [3072, 3072], P('outer', ('inner', 'head')), may hold values from -0.109375 to 0.109375
- out_weight: bfloat16 [3072, 3072], P(('inner', 'head'), 'outer'), may hold values from -0.109375 to 0.109375
- query_gain: float32 [128], replicated, may hold values from 1 to 18, as said below
- key_gain: float32 [128], replicated, may hold values from 1 to 18, as said below
Outputs:
- attended: bfloat16 [2, 4096, 3072], P('clip', ('outer', 'inner', 'head')), parts along dimension 0
The draws below stay inside these ranges and needn't reach their ends.
There are 2 independent parts, one for each index of `clip`. The reference program is written for one: setup_inputs(seed, part) draws one part's arguments, and reference() takes and returns one part's arrays. A program takes and returns all parts, laid end to end along the dimension named above; an argument that names none is the same for every part. Nothing has to cross between parts.
Inputs may be any that keep to these rules, and one draw needn't show every extreme that they name: `query_gain`: 128 positive scales. `key_gain`: 128 positive scales.
All inputs are finite; a program needn't handle non-finite values.
Results may differ from the reference program's by a relative error of at most 0.015.
The reference program's roundings to bfloat16 on the way (of `modulated`, `value_heads`, `mixed` and `group_term`) count: a program that leaves them out, or rounds other values in their place, can miss the bound.
Values may be sent and summed in bfloat16 or wider, within the bound.
A program may use at most 192 MiB of HBM per device.

```python
import math
import jax
import jax.numpy as jnp
from jax import lax

D = 3072
HEADS = 24
HD = 128
S = 4096
CLIPS = 1
N_INNER = 2
N_HEAD = 2


def base_gain(key):
    lower_log = jnp.log(jnp.float32(1.0))
    upper_log = jnp.log(jnp.float32(2.0))
    return jnp.exp(jax.random.uniform(key, (HD,), jnp.float32, lower_log, upper_log))


def draw_query_gain(key, part):
    gain_values = base_gain(jax.random.fold_in(key, 1))
    return gain_values


def draw_key_gain(key, part):
    gain_values = base_gain(jax.random.fold_in(key, 2))
    return gain_values


def levels(stream_key, dims, cuts, least, high):
    factor_of = 1.0
    for position, shards_of in cuts:
        steps = jax.random.uniform(jax.random.fold_in(jax.random.fold_in(stream_key, 6), position), (shards_of,), jnp.float32, least / len(cuts), high / len(cuts))
        factor_of = factor_of * jnp.repeat(jnp.exp(steps), dims[position] // shards_of).reshape((-1,) + (1,) * (len(dims) - 1 - position))
    return factor_of


def noise(rng, dims, scale, limit, shards=(), held_as=jnp.bfloat16):
    entries = jax.random.normal(rng, dims, jnp.float32) * scale
    if len(shards) > 0:
        entries = levels(rng, dims, shards, -0.22, 0.18) * entries
    return jnp.clip(entries, min=-limit, max=limit).astype(held_as)


def setup_inputs(seed: int = 0, part: int = 0) -> dict:
    keys = jax.random.split(jax.random.key(seed), 11)
    own_keys = jax.random.split(jax.random.fold_in(keys[10], part), 11)
    return {
        "tokens": noise(own_keys[0], (CLIPS, S, D), 1.0, 6.0, ((1, 16),)),
        "shift_mod": noise(own_keys[1], (CLIPS, D), 0.5, 3.0, (), jnp.float32),
        "scale_mod": noise(own_keys[2], (CLIPS, D), 0.3, 1.5, (), jnp.float32),
        "gate_mod": jnp.clip(jax.random.uniform(own_keys[3], (CLIPS, D), jnp.float32, 0.5, 2.0), 0.5, 2.0),
        "query_weight": noise(keys[4], (D, HEADS * HD), D ** -0.5, 0.109375, ((0, 4), (1, 4))),
        "key_weight": noise(keys[5], (D, HEADS * HD), D ** -0.5, 0.109375, ((0, 4), (1, 4))),
        "value_weight": noise(keys[6], (D, HEADS * HD), D ** -0.5, 0.109375, ((0, 4), (1, 4))),
        "out_weight": noise(keys[7], (HEADS * HD, D), (HEADS * HD) ** -0.5, 0.109375, ((0, 4), (1, 4))),
        "query_gain": draw_query_gain(jax.random.fold_in(keys[10], 71), part),
        "key_gain": draw_key_gain(jax.random.fold_in(keys[10], 71), part),
    }


EPSILON = 1e-06

def modulate(tokens, shift_mod, scale_mod):
    values = tokens.astype(jnp.float32)
    center = lax.optimization_barrier(jnp.mean(values, axis=-1, keepdims=True))
    spread = lax.optimization_barrier(jnp.mean(jnp.square(values - center), axis=-1, keepdims=True))
    normed = (values - center) / jnp.sqrt(spread + EPSILON)
    return (normed * (1.0 + scale_mod[:, None, :]) + shift_mod[:, None, :]).astype(jnp.bfloat16)

def head_norm(projected, gain_vec, head_dim):
    shaped = projected.reshape(projected.shape[:-1] + (projected.shape[-1] // head_dim, head_dim))
    mean_square = lax.optimization_barrier(jnp.mean(jnp.square(shaped), axis=-1, keepdims=True))
    return (shaped / jnp.sqrt(mean_square + EPSILON) * gain_vec).astype(jnp.bfloat16)

def one_head(operands):
    query_one, key_one, value_one = operands
    scores = jnp.einsum('cqd,ckd->cqk', query_one.astype(jnp.float32), key_one.astype(jnp.float32), precision=lax.Precision.HIGHEST) / math.sqrt(HD)
    row_max = lax.optimization_barrier(jnp.max(scores, axis=-1, keepdims=True))
    weights = jnp.exp(scores - row_max)
    row_total = lax.optimization_barrier(jnp.sum(weights, axis=-1, keepdims=True))
    rounded = lax.optimization_barrier(weights.astype(jnp.bfloat16))
    mixed_values = jnp.einsum('cqk,ckd->cqd', rounded.astype(jnp.float32), value_one.astype(jnp.float32), precision=lax.Precision.HIGHEST)
    return mixed_values / row_total

def reference(tokens, shift_mod, scale_mod, gate_mod, query_weight, key_weight, value_weight, out_weight, query_gain, key_gain):
    clip_count = tokens.shape[0]
    all_cols = HEADS * HD
    modulated = modulate(tokens, shift_mod, scale_mod).reshape(clip_count * S, D)
    query_proj = jnp.dot(modulated, query_weight, preferred_element_type=jnp.float32)
    key_proj = jnp.dot(modulated, key_weight, preferred_element_type=jnp.float32)
    value_proj = jnp.dot(modulated, value_weight, preferred_element_type=jnp.float32)
    query_heads = lax.optimization_barrier(head_norm(query_proj.reshape(clip_count, S, all_cols), query_gain, HD))
    key_heads = lax.optimization_barrier(head_norm(key_proj.reshape(clip_count, S, all_cols), key_gain, HD))
    value_heads = lax.optimization_barrier(value_proj.astype(jnp.bfloat16).reshape(clip_count, S, HEADS, HD))
    stacked = (jnp.transpose(query_heads, (2, 0, 1, 3)), jnp.transpose(key_heads, (2, 0, 1, 3)), jnp.transpose(value_heads, (2, 0, 1, 3)))
    head_out = lax.map(one_head, stacked)
    mixed = jnp.transpose(head_out, (1, 2, 0, 3)).reshape(clip_count * S, all_cols).astype(jnp.bfloat16)
    groups = N_INNER * N_HEAD
    group_width = all_cols // groups
    summed = jnp.zeros((clip_count * S, D), jnp.float32)
    for group_index in range(groups):
        lower = group_index * group_width
        group_term = jnp.dot(mixed[:, lower:lower + group_width], out_weight[lower:lower + group_width, :], preferred_element_type=jnp.float32).astype(jnp.bfloat16)
        group_term = lax.optimization_barrier(group_term)
        summed = summed + group_term.astype(jnp.float32)
    return (summed.reshape(clip_count, S, D) * gate_mod[:, None, :]).astype(jnp.bfloat16)
```

```python
import functools
import math

import jax
import jax.numpy as jnp
from jax import lax
from jax.experimental import pallas as pl
from jax.experimental.pallas import tpu as pltpu
from jax.sharding import PartitionSpec as P

EPSILON = 1e-06


def modulate(tokens, shift_mod, scale_mod):
    values = tokens.astype(jnp.float32)
    center = jnp.mean(values, axis=-1, keepdims=True)
    spread = jnp.mean(jnp.square(values - center), axis=-1, keepdims=True)
    normed = (values - center) / jnp.sqrt(spread + EPSILON)
    return (normed * (1.0 + scale_mod[:, None, :]) + shift_mod[:, None, :]).astype(jnp.bfloat16)


def head_norm(projected, gain_vec, head_dim):
    shaped = projected.reshape(projected.shape[:-1] + (projected.shape[-1] // head_dim, head_dim))
    mean_square = jnp.mean(jnp.square(shaped), axis=-1, keepdims=True)
    return (shaped / jnp.sqrt(mean_square + EPSILON) * gain_vec).astype(jnp.bfloat16)


def per_device(
    tokens,
    shift_mod,
    scale_mod,
    gate_mod,
    query_weight,
    key_weight,
    value_weight,
    out_weight,
    query_gain,
    key_gain,
):
    head_dim = query_gain.shape[0]
    modulated = modulate(tokens, shift_mod, scale_mod)
    gathered = lax.all_gather(modulated, ("inner", "head"), axis=1, tiled=True)
    clip_count, row_count, model_width = gathered.shape
    flattened = gathered.reshape(clip_count * row_count, model_width)
    local_cols = query_weight.shape[1]
    head_count = local_cols // head_dim
    full_query, full_key, full_value = (
        lax.all_gather(query_weight, "outer", axis=0, tiled=True),
        lax.all_gather(key_weight, "outer", axis=0, tiled=True),
        lax.all_gather(value_weight, "outer", axis=0, tiled=True),
    )
    query_proj = jnp.dot(flattened, full_query, preferred_element_type=jnp.float32)
    key_proj = jnp.dot(flattened, full_key, preferred_element_type=jnp.float32)
    value_proj = jnp.dot(flattened, full_value, preferred_element_type=jnp.float32)
    query_heads = head_norm(
        query_proj.reshape(clip_count, row_count, local_cols), query_gain, head_dim
    )
    key_send = head_norm(key_proj.reshape(clip_count, row_count, local_cols), key_gain, head_dim)
    key_send = key_send.reshape(clip_count, row_count, local_cols)
    value_send = value_proj.astype(jnp.bfloat16).reshape(clip_count, row_count, local_cols)
    root_size = math.sqrt(head_dim)
    full_out = lax.all_gather(out_weight, "outer", axis=1, tiled=True)
    running_max = jnp.full((clip_count, head_count, row_count), -1e30, jnp.float32)
    key_piece = lax.all_gather(key_send, "outer", axis=1, tiled=True)
    value_piece = lax.all_gather(value_send, "outer", axis=1, tiled=True)
    key_count = key_piece.shape[1]
    key_piece = key_piece.reshape(clip_count, key_count, head_count, head_dim)
    value_piece = value_piece.reshape(clip_count, key_count, head_count, head_dim)
    scores = (
        jnp.einsum("cqhd,ckhd->chqk", query_heads, key_piece, preferred_element_type=jnp.float32)
        / root_size
    )
    new_max = jnp.maximum(running_max, jnp.max(scores, axis=-1))
    weights = jnp.exp(scores - new_max[..., None])
    new_sum = jnp.sum(weights, axis=-1)
    new_acc = jnp.einsum(
        "chqk,ckhd->chqd",
        weights.astype(jnp.bfloat16),
        value_piece,
        preferred_element_type=jnp.float32,
    )
    head_out = new_acc / new_sum[..., None]
    mixed = (
        jnp.transpose(head_out, (0, 2, 1, 3))
        .reshape(clip_count * row_count, local_cols)
        .astype(jnp.bfloat16)
    )
    partial_value = jnp.dot(mixed, full_out, preferred_element_type=jnp.float32).reshape(
        clip_count, row_count, -1
    )
    summed = lax.psum_scatter(
        partial_value.astype(jnp.bfloat16), ("inner", "head"), scatter_dimension=1, tiled=True
    ).astype(jnp.float32)
    return (summed * gate_mod[:, None, :]).astype(jnp.bfloat16)


def sublayer(
    nz,
    head_dim,
    tokens,
    shift_mod,
    scale_mod,
    gate_mod,
    query_gain,
    key_gain,
    query_weight,
    key_weight,
    value_weight,
    out_weight,
    out,
    weights,
    gathered,
    queries,
    kv,
    out_full,
    mixed,
    staged,
    w_send,
    w_recv,
    wx_send,
    wx_recv,
    wy_send,
    wy_recv,
    t_own,
    t_fwd,
    t_recv,
    s_send,
    s_recv,
    kv_send,
    kv_recv,
    m_send,
    m_recv,
    p_local,
    p_send,
    p_recv,
    o_own,
    o_fwd,
    o_recv,
    oy_send,
    oy_recv,
    ox_send,
    ox_recv,
    od_send,
    od_recv,
    os_send,
    os_recv,
):
    y, z = lax.axis_index("clip"), lax.axis_index("outer")
    x, h = lax.axis_index("inner"), lax.axis_index("head")
    rows, width = tokens.shape
    depth = query_weight.shape[0]
    half = depth // 2
    cols = queries.shape[0] * head_dim
    heads = queries.shape[0]
    per_core = nz // 2
    group, block_cols = out_weight.shape
    group_half = group // 2
    high = z // (nz // 2)
    inner, outer = z + 1 - 2 * high, z - 1 + 2 * high
    middle = jnp.logical_and(z > 0, z < nz - 1)
    end = jnp.logical_not(middle)
    primary = h == x
    other = jnp.logical_not(primary)

    sibling, across_y, across_x = {"head": 1 - h}, {"clip": 1 - y}, {"inner": 1 - x}
    sends = []

    def block(t):
        first, odd = 1 - t // 2, t % 2
        return (
            first * (1 - odd) * z
            + first * odd * (1 - z + 4 * high)
            + (1 - first) * ((1 - high) * t + high * (3 - t))
        )

    def when(cond, run):
        if cond is None:
            run()
        else:
            pl.when(cond)(run)

    def send(src, dst, send_sem, recv_sem, device, cond=None):
        def make():
            return pltpu.make_async_remote_copy(
                src_ref=src(),
                dst_ref=dst(),
                send_sem=send_sem,
                recv_sem=recv_sem,
                device_id=device,
                device_id_type=pl.DeviceIdType.MESH,
            )

        when(cond, lambda: make().start())
        return make

    def post(ref, index, send_sem, recv_sem, device, cond=None, source=None):
        dst = lambda: ref.at[index()]
        src = dst if source is None else source
        made = send(src, dst, send_sem, recv_sem, device, cond)
        sends.append((cond, made))

    def arrive(view, sem):
        pltpu.make_async_copy(view, view, sem).wait()

    barrier = pltpu.get_barrier_semaphore()

    def greet(device):
        pl.semaphore_signal(
            barrier, inc=1, device_id=device, device_id_type=pl.DeviceIdType.MESH
        )

    for zs in range(nz):
        for hs in range(2):
            away = jnp.logical_or(z != zs, h != hs)
            pl.when(away)(lambda zs=zs, hs=hs: greet({"outer": zs, "head": hs}))
    greet(across_y)
    greet(across_x)
    pl.semaphore_wait(barrier, 2 * nz + 1)

    for k in range(per_core):
        target = h * per_core + k
        local = jnp.logical_and(target == z, primary)
        remote = jnp.logical_not(local)
        for m, weight in enumerate((query_weight, key_weight, value_weight)):
            src = weight.at[pl.ds(y * half, half), pl.ds(k * cols, cols)]
            index = (pl.ds(z * depth + y * half, half), pl.ds(m * cols, cols))
            pl.when(local)(
                lambda src=src, index=index, m=m: pltpu.make_async_copy(
                    src, weights.at[index], w_recv.at[z, m]
                ).start()
            )
            post(
                weights,
                lambda index=index: index,
                w_send.at[k, m],
                w_recv.at[z, m],
                {"outer": target, "head": x},
                remote,
                lambda src=src: src,
            )

    own_out = pltpu.make_async_copy(
        out_weight, out_full.at[z, pl.ds((2 * x + h) * group, group)], p_local
    )
    own_out.start()

    slab = 32 if rows % 32 == 0 else 16

    @pl.loop(0, rows // slab)
    def _(r):
        values = tokens[pl.ds(r * slab, slab), :].astype(jnp.float32)
        center = jnp.mean(values, axis=-1, keepdims=True)
        moved = values - center
        spread = jnp.mean(moved * moved, axis=-1, keepdims=True)
        normed = moved * (1.0 / jnp.sqrt(spread + EPSILON))
        changed = normed * (1.0 + scale_mod[...]) + shift_mod[...]
        gathered[z, pl.ds(h * rows + r * slab, slab), :] = changed.astype(jnp.bfloat16)

    def shard(b):
        return lambda: (b, pl.ds(h * rows, rows))

    def sibling_shard(b):
        return gathered.at[b, pl.ds((1 - h) * rows, rows)]

    def near(b):
        return lambda: (pl.ds(b * depth + y * half, half), slice(None))

    def far(b):
        return weights.at[pl.ds(b * depth + (1 - y) * half, half), :]

    b = [block(t) for t in range(nz)]
    post(gathered, shard(z), t_own.at[0], t_recv.at[z], {"outer": inner})
    post(gathered, shard(z), t_own.at[1], t_recv.at[z], {"outer": outer}, middle)
    post(gathered, shard(z), s_send.at[z], s_recv.at[z], sibling)

    def part(bt, gx, gy):
        start = (2 * gx + h) * group + gy * group_half
        return lambda: (bt, pl.ds(start, group_half))

    def out_source():
        return out_weight.at[pl.ds(y * group_half, group_half), :]

    post(
        out_full, part(z, x, y), o_own.at[0], o_recv.at[z], {"outer": inner}, end, out_source
    )

    def pass_on(bt):
        post(weights, near(bt), wy_send.at[bt], wy_recv.at[bt], across_y)

    for bt in b:
        def take(bt=bt):
            for m in range(3):
                index = (pl.ds(bt * depth + y * half, half), pl.ds(m * cols, cols))
                arrive(weights.at[index], w_recv.at[bt, m])

        pl.when(primary)(take)
        post(weights, near(bt), wx_send.at[bt], wx_recv.at[bt], across_x, primary)
        pl.when(other)(lambda bt=bt: arrive(weights.at[near(bt)()], wx_recv.at[bt]))
        pass_on(bt)

    own_index = lambda: (z, pl.ds((2 * x + h) * group, group))
    post(out_full, own_index, p_send.at[0], p_recv.at[0], across_x, None, lambda: out_weight)
    post(out_full, own_index, p_send.at[1], p_recv.at[1], sibling, None, lambda: out_weight)

    def take_tokens(t, cond=None):
        bt = b[t]
        moves = middle if cond is None else jnp.logical_and(middle, cond)
        when(cond, lambda: arrive(gathered.at[shard(bt)()], t_recv.at[bt]))
        target = inner if t == 1 else outer

        def go():
            send(
                lambda: gathered.at[shard(bt)()],
                lambda: gathered.at[shard(bt)()],
                t_fwd.at[t],
                t_recv.at[bt],
                {"outer": target},
            )

        def side():
            send(
                lambda: gathered.at[shard(bt)()],
                lambda: gathered.at[shard(bt)()],
                s_send.at[bt],
                s_recv.at[bt],
                sibling,
            )

        pl.when(moves)(go)
        when(cond, side)

    take_tokens(1)
    post(
        out_full, part(z, x, y), o_own.at[0], o_recv.at[z], {"outer": inner}, middle, out_source
    )
    take_tokens(2, middle)
    for bt in b:
        arrive(far(bt), wy_recv.at[bt])

    def normed_head(projected, gain):
        square = jnp.mean(projected * projected, axis=-1, keepdims=True)
        return (projected * (1.0 / jnp.sqrt(square + EPSILON)) * gain).astype(jnp.bfloat16)

    def project(bt):
        @pl.loop(0, 2)
        def _(r):
            here = pl.ds(pl.multiple_of(r * rows, rows), rows)
            piece = gathered[bt, here, :]
            both = jnp.dot(
                piece, weights[:, : 2 * cols], preferred_element_type=jnp.float32
            )
            for i in range(heads):
                lo = i * head_dim
                queries[i, bt, here, :] = normed_head(
                    both[:, lo : lo + head_dim], query_gain[...]
                )
                kv[0, i, x * nz + bt, here, :] = normed_head(
                    both[:, cols + lo : cols + lo + head_dim], key_gain[...]
                )
            value = jnp.dot(
                piece, weights[:, 2 * cols :], preferred_element_type=jnp.float32
            ).astype(jnp.bfloat16)
            for i in range(heads):
                lo = i * head_dim
                kv[1, i, x * nz + bt, here, :] = value[:, lo : lo + head_dim]

        post(
            kv,
            lambda: (slice(None), slice(None), x * nz + bt),
            kv_send.at[bt],
            kv_recv.at[bt],
            across_x,
        )

    def out_near(t, cond=None):
        bt = b[t]

        def run():
            mine = part(bt, x, y)
            arrive(out_full.at[mine()], o_recv.at[bt])
            target = inner if t == 1 else outer
            view = lambda: out_full.at[mine()]
            pl.when(middle)(
                lambda: send(view, view, o_fwd.at[t], o_recv.at[bt], {"outer": target}) and None
            )
            send(view, view, oy_send.at[t], oy_recv.at[t], across_y)
            send(view, view, ox_send.at[t], ox_recv.at[t], across_x)
            send(view, view, os_send.at[t, 0], os_recv.at[t, 0], sibling)

        when(cond, run)

    def out_second(t):
        bt = b[t]
        side, over = part(bt, x, 1 - y), part(bt, 1 - x, y)
        side_view, over_view = lambda: out_full.at[side()], lambda: out_full.at[over()]
        arrive(side_view(), oy_recv.at[t])
        if t == 1:
            send(side_view, side_view, od_send.at[t], od_recv.at[t], across_x)
        send(side_view, side_view, os_send.at[t, 1], os_recv.at[t, 1], sibling)
        arrive(over_view(), ox_recv.at[t])
        if t > 1:
            send(over_view, over_view, od_send.at[t], od_recv.at[t], across_y)
        send(over_view, over_view, os_send.at[t, 2], os_recv.at[t, 2], sibling)

    def out_third(t):
        last = part(b[t], 1 - x, 1 - y)
        view = lambda: out_full.at[last()]
        arrive(view(), od_recv.at[t])
        send(view, view, os_send.at[t, 3], os_recv.at[t, 3], sibling)

    arrive(sibling_shard(b[0]), s_recv.at[b[0]])
    project(b[0])
    arrive(sibling_shard(b[1]), s_recv.at[b[1]])
    project(b[1])
    take_tokens(2, end)
    arrive(sibling_shard(b[2]), s_recv.at[b[2]])
    project(b[2])
    take_tokens(3)
    post(
        out_full, part(z, x, y), o_own.at[1], o_recv.at[z], {"outer": outer}, middle, out_source
    )
    out_near(1, middle)
    cross = lambda: (z, pl.ds((2 * (1 - x) + h) * group, group))
    arrive(out_full.at[cross()], p_recv.at[0])
    post(out_full, cross, p_send.at[2], p_recv.at[2], sibling)
    arrive(sibling_shard(b[3]), s_recv.at[b[3]])
    project(b[3])
    for bt in b:
        arrive(kv.at[:, :, (1 - x) * nz + bt], kv_recv.at[bt])

    factor = math.log2(math.e) / math.sqrt(head_dim)
    key_blocks, key_rows = kv.shape[2], kv.shape[3]
    span = 2 if key_blocks % 2 == 0 else 1

    def attend_rows(query, i):
        total = None
        for c in range(0, key_blocks, span):
            keys = kv[0, i, c : c + span].reshape(span * key_rows, head_dim)
            values = kv[1, i, c : c + span].reshape(span * key_rows, head_dim)
            scores = lax.dot_general(
                query, keys, (((1,), (1,)), ((), ())), preferred_element_type=jnp.float32
            )
            peak = jnp.max(scores, axis=-1, keepdims=True)
            if c:
                peak = jnp.maximum(top, peak)
            probs = jnp.exp2((scores - peak) * factor)
            fresh = jnp.sum(probs, axis=-1, keepdims=True)
            gained = jnp.dot(
                probs.astype(jnp.bfloat16), values, preferred_element_type=jnp.float32
            )
            if c:
                shrink = jnp.exp2((top - peak) * factor)
                total, result = total * shrink + fresh, result * shrink + gained
            else:
                total, result = fresh, gained
            top = peak
        return (result / total).astype(jnp.bfloat16)

    def place():
        return (slice(None), pl.ds((h * nz + z) * cols, cols))

    duties = {
        1: lambda: (out_near(1, end), out_near(2, middle)),
        3: lambda: (out_near(2, end), out_near(3, middle), out_second(1)),
        5: lambda: (out_near(3, end), out_second(2), out_third(1)),
        7: lambda: (out_second(3), out_third(2)),
    }

    @pl.loop(0, 2 * nz)
    def _(j):
        for at, duty in duties.items():
            pl.when(j == at)(lambda duty=duty: duty() and None)
        bt = block(nz - 1 - j // 2)
        core = (j % 2) * h + (1 - j % 2) * (1 - h)

        @pl.loop(0, heads)
        def _(i):
            query = queries[i, bt, pl.ds(core * rows, rows), :]
            staged[bt, core, :, pl.ds(pl.multiple_of(i * head_dim, head_dim), head_dim)] = (
                attend_rows(query, i)
            )

        self_place = jnp.logical_and(bt == z, core == h)

        def keep():
            mixed[place()] = staged[bt, core]

        pl.when(self_place)(keep)

        def give():
            send(
                lambda: staged.at[bt, core],
                lambda: mixed.at[place()],
                m_send.at[bt, core],
                m_recv.at[h * nz + z],
                {"outer": bt, "head": core},
            )

        pl.when(jnp.logical_not(self_place))(give)

    out_third(3)
    for zs in range(nz):
        for hs in range(2):
            k = hs * nz + zs
            pl.when(jnp.logical_or(z != zs, h != hs))(
                lambda k=k: arrive(mixed.at[:, k * cols : (k + 1) * cols], m_recv.at[k])
            )

    def sibling_part(bt, gx, gy):
        start = (2 * gx + 1 - h) * group + gy * group_half
        return out_full.at[bt, pl.ds(start, group_half)]

    own_out.wait()
    for gx, n in ((x, 1), (1 - x, 2)):
        arrive(out_full.at[z, pl.ds((2 * gx + 1 - h) * group, group)], p_recv.at[n])

    for t in range(nz):
        bt = b[t]
        if t:
            for n, (gx, gy) in enumerate(((x, y), (x, 1 - y), (1 - x, y), (1 - x, 1 - y))):
                arrive(sibling_part(bt, gx, gy), os_recv.at[t, n])
        summed = jnp.zeros((rows, block_cols), jnp.float32)
        for g in range(4):
            term = jnp.dot(
                mixed[:, g * group : (g + 1) * group],
                out_full[bt, g * group : (g + 1) * group, :],
                preferred_element_type=jnp.float32,
            )
            summed = summed + term.astype(jnp.bfloat16).astype(jnp.float32)
        here = pl.ds(pl.multiple_of(bt * block_cols, block_cols), block_cols)
        out[:, here] = (summed * gate_mod[:, here]).astype(jnp.bfloat16)

    for cond, made in sends:
        when(cond, lambda made=made: made().wait_send())

    def sent(view, sem):
        pltpu.make_async_copy(view, view, sem).wait()

    for t in range(1, nz):
        bt = b[t]
        tok = gathered.at[shard(bt)()]
        pl.when(middle)(lambda tok=tok, t=t: sent(tok, t_fwd.at[t]))
        sent(tok, s_send.at[bt])
        piece = out_full.at[part(bt, x, y)()]
        pl.when(middle)(lambda piece=piece, t=t: sent(piece, o_fwd.at[t]))
        sent(piece, oy_send.at[t])
        sent(piece, ox_send.at[t])
        sent(piece, od_send.at[t])
        for n in range(4):
            sent(piece, os_send.at[t, n])
    for zs in range(nz):
        for hs in range(2):
            pl.when(jnp.logical_or(z != zs, h != hs))(
                lambda zs=zs, hs=hs: sent(staged.at[zs, hs], m_send.at[zs, hs])
            )


def fused(nz, tokens, shift_mod, scale_mod, gate_mod, *rest):
    wq, wk, wv, wo, query_gain, key_gain = rest
    _, rows, width = tokens.shape
    head_dim = query_gain.shape[0]
    depth, group_cols = wq.shape
    heads = 4 * group_cols // head_dim // (2 * nz)
    cols = heads * head_dim
    dma = lambda *shape: pltpu.SemaphoreType.DMA(shape)
    vmem = pl.BlockSpec(memory_space=pltpu.VMEM)
    anywhere = pl.BlockSpec(memory_space=pl.ANY)
    result = pl.pallas_call(
        functools.partial(sublayer, nz, head_dim),
        out_shape=jax.ShapeDtypeStruct((rows, width), jnp.bfloat16),
        in_specs=[vmem] * 6 + [anywhere] * 4,
        out_specs=vmem,
        scratch_shapes=[
            pltpu.VMEM((width, 3 * cols), jnp.bfloat16),
            pltpu.VMEM((nz, 2 * rows, width), jnp.bfloat16),
            pltpu.VMEM((heads, nz, 2 * rows, head_dim), jnp.bfloat16),
            pltpu.VMEM((2, heads, 2 * nz, 2 * rows, head_dim), jnp.bfloat16),
            pltpu.VMEM((nz, 4 * wo.shape[0], wo.shape[1]), jnp.bfloat16),
            pltpu.VMEM((rows, width), jnp.bfloat16),
            pltpu.VMEM((nz, 2, rows, cols), jnp.bfloat16),
            dma(nz // 2, 3),
            dma(nz, 3),
            dma(nz),
            dma(nz),
            dma(nz),
            dma(nz),
            dma(2),
            dma(nz),
            dma(nz),
            dma(nz),
            dma(nz),
            dma(nz),
            dma(nz),
            dma(nz, 2),
            dma(2 * nz),
            pltpu.SemaphoreType.DMA,
            dma(3),
            dma(3),
            dma(2),
            dma(nz),
            dma(nz),
            dma(nz),
            dma(nz),
            dma(nz),
            dma(nz),
            dma(nz),
            dma(nz),
            dma(nz, 4),
            dma(nz, 4),
        ],
        compiler_params=pltpu.CompilerParams(
            collective_id=0, has_side_effects=True, vmem_limit_bytes=67043328
        ),
        name="sublayer",
    )(
        tokens[0],
        shift_mod,
        scale_mod,
        gate_mod,
        query_gain[None],
        key_gain[None],
        wq,
        wk,
        wv,
        wo,
    )
    return result[None]


def fits(mesh, args):
    sizes = mesh.shape
    head_dim, (depth, group_cols) = args[8].shape[0], args[4].shape
    nz = sizes["outer"]
    return (
        sizes["inner"] == 2
        and sizes["head"] == 2
        and sizes["clip"] == 2
        and nz == 4
        and args[0].shape[0] == 1
        and args[0].shape[1] % 16 == 0
        and head_dim % 128 == 0
        and (4 * group_cols) % (2 * nz * head_dim) == 0
        and depth % 32 == 0
    )


def solution(mesh):
    in_specs = (
        P("clip", ("outer", "inner", "head"), None),
        P("clip", None),
        P("clip", None),
        P("clip", None),
        P("outer", ("inner", "head")),
        P("outer", ("inner", "head")),
        P("outer", ("inner", "head")),
        P(("inner", "head"), "outer"),
        P(),
        P(),
    )
    out_specs = P("clip", ("outer", "inner", "head"), None)

    def body(*args):
        if fits(mesh, args):
            return fused(mesh.shape["outer"], *args)
        return per_device(*args)

    return jax.shard_map(
        body, mesh=mesh, in_specs=in_specs, out_specs=out_specs, check_vma=False
    )
```

```python
import functools
import math

import jax
import jax.numpy as jnp
from jax import lax
from jax.experimental import pallas as pl
from jax.experimental.pallas import tpu as pltpu
from jax.sharding import PartitionSpec as P

EPSILON = 1e-06


def modulate(tokens, shift_mod, scale_mod):
    values = tokens.astype(jnp.float32)
    center = jnp.mean(values, axis=-1, keepdims=True)
    spread = jnp.mean(jnp.square(values - center), axis=-1, keepdims=True)
    normed = (values - center) / jnp.sqrt(spread + EPSILON)
    return (normed * (1.0 + scale_mod[:, None, :]) + shift_mod[:, None, :]).astype(jnp.bfloat16)


def head_norm(projected, gain_vec, head_dim):
    shaped = projected.reshape(projected.shape[:-1] + (projected.shape[-1] // head_dim, head_dim))
    mean_square = jnp.mean(jnp.square(shaped), axis=-1, keepdims=True)
    return (shaped / jnp.sqrt(mean_square + EPSILON) * gain_vec).astype(jnp.bfloat16)


def per_device(
    tokens,
    shift_mod,
    scale_mod,
    gate_mod,
    query_weight,
    key_weight,
    value_weight,
    out_weight,
    query_gain,
    key_gain,
):
    head_dim = query_gain.shape[0]
    modulated = modulate(tokens, shift_mod, scale_mod)
    gathered = lax.all_gather(modulated, ("inner", "head"), axis=1, tiled=True)
    clip_count, row_count, model_width = gathered.shape
    flattened = gathered.reshape(clip_count * row_count, model_width)
    local_cols = query_weight.shape[1]
    head_count = local_cols // head_dim
    full_query, full_key, full_value = (
        lax.all_gather(query_weight, "outer", axis=0, tiled=True),
        lax.all_gather(key_weight, "outer", axis=0, tiled=True),
        lax.all_gather(value_weight, "outer", axis=0, tiled=True),
    )
    query_proj = jnp.dot(flattened, full_query, preferred_element_type=jnp.float32)
    key_proj = jnp.dot(flattened, full_key, preferred_element_type=jnp.float32)
    value_proj = jnp.dot(flattened, full_value, preferred_element_type=jnp.float32)
    query_heads = head_norm(
        query_proj.reshape(clip_count, row_count, local_cols), query_gain, head_dim
    )
    key_send = head_norm(key_proj.reshape(clip_count, row_count, local_cols), key_gain, head_dim)
    key_send = key_send.reshape(clip_count, row_count, local_cols)
    value_send = value_proj.astype(jnp.bfloat16).reshape(clip_count, row_count, local_cols)
    root_size = math.sqrt(head_dim)
    full_out = lax.all_gather(out_weight, "outer", axis=1, tiled=True)
    running_max = jnp.full((clip_count, head_count, row_count), -1e30, jnp.float32)
    key_piece = lax.all_gather(key_send, "outer", axis=1, tiled=True)
    value_piece = lax.all_gather(value_send, "outer", axis=1, tiled=True)
    key_count = key_piece.shape[1]
    key_piece = key_piece.reshape(clip_count, key_count, head_count, head_dim)
    value_piece = value_piece.reshape(clip_count, key_count, head_count, head_dim)
    scores = (
        jnp.einsum("cqhd,ckhd->chqk", query_heads, key_piece, preferred_element_type=jnp.float32)
        / root_size
    )
    new_max = jnp.maximum(running_max, jnp.max(scores, axis=-1))
    weights = jnp.exp(scores - new_max[..., None])
    new_sum = jnp.sum(weights, axis=-1)
    new_acc = jnp.einsum(
        "chqk,ckhd->chqd",
        weights.astype(jnp.bfloat16),
        value_piece,
        preferred_element_type=jnp.float32,
    )
    head_out = new_acc / new_sum[..., None]
    mixed = (
        jnp.transpose(head_out, (0, 2, 1, 3))
        .reshape(clip_count * row_count, local_cols)
        .astype(jnp.bfloat16)
    )
    partial_value = jnp.dot(mixed, full_out, preferred_element_type=jnp.float32).reshape(
        clip_count, row_count, -1
    )
    summed = lax.psum_scatter(
        partial_value.astype(jnp.bfloat16), ("inner", "head"), scatter_dimension=1, tiled=True
    ).astype(jnp.float32)
    return (summed * gate_mod[:, None, :]).astype(jnp.bfloat16)


def sublayer(
    nz,
    head_dim,
    tokens,
    shift_mod,
    scale_mod,
    gate_mod,
    query_gain,
    key_gain,
    query_weight,
    key_weight,
    value_weight,
    out_weight,
    out,
    weights,
    gathered,
    queries,
    kv,
    out_full,
    mixed,
    staged,
    w_send,
    w_recv,
    wx_send,
    wx_recv,
    wy_send,
    wy_recv,
    t_own,
    t_fwd,
    t_recv,
    s_send,
    s_recv,
    kv_send,
    kv_recv,
    m_send,
    m_recv,
    p_local,
    p_send,
    p_recv,
    o_own,
    o_fwd,
    o_recv,
    oy_send,
    oy_recv,
    ox_send,
    ox_recv,
    od_send,
    od_recv,
    os_send,
    os_recv,
):
    y, z = lax.axis_index("clip"), lax.axis_index("outer")
    x, h = lax.axis_index("inner"), lax.axis_index("head")
    rows, width = tokens.shape
    depth = query_weight.shape[0]
    half = depth // 2
    cols = queries.shape[0] * head_dim
    heads = queries.shape[0]
    per_core = nz // 2
    group, block_cols = out_weight.shape
    group_half = group // 2
    high = z // (nz // 2)
    inner, outer = z + 1 - 2 * high, z - 1 + 2 * high
    middle = jnp.logical_and(z > 0, z < nz - 1)
    end = jnp.logical_not(middle)
    primary = h == x
    other = jnp.logical_not(primary)

    sibling, across_y, across_x = {"head": 1 - h}, {"clip": 1 - y}, {"inner": 1 - x}
    sends = []

    def block(t):
        first, odd = 1 - t // 2, t % 2
        return (
            first * (1 - odd) * z
            + first * odd * (1 - z + 4 * high)
            + (1 - first) * ((1 - high) * t + high * (3 - t))
        )

    def when(cond, run):
        if cond is None:
            run()
        else:
            pl.when(cond)(run)

    def send(src, dst, send_sem, recv_sem, device, cond=None):
        def make():
            return pltpu.make_async_remote_copy(
                src_ref=src(),
                dst_ref=dst(),
                send_sem=send_sem,
                recv_sem=recv_sem,
                device_id=device,
                device_id_type=pl.DeviceIdType.MESH,
            )

        when(cond, lambda: make().start())
        return make

    def post(ref, index, send_sem, recv_sem, device, cond=None, source=None):
        dst = lambda: ref.at[index()]
        src = dst if source is None else source
        made = send(src, dst, send_sem, recv_sem, device, cond)
        sends.append((cond, made))

    def arrive(view, sem):
        pltpu.make_async_copy(view, view, sem).wait()

    barrier = pltpu.get_barrier_semaphore()

    def greet(device):
        pl.semaphore_signal(
            barrier, inc=1, device_id=device, device_id_type=pl.DeviceIdType.MESH
        )

    for zs in range(nz):
        for hs in range(2):
            away = jnp.logical_or(z != zs, h != hs)
            pl.when(away)(lambda zs=zs, hs=hs: greet({"outer": zs, "head": hs}))
    greet(across_y)
    greet(across_x)
    own_out = pltpu.make_async_copy(
        out_weight, out_full.at[z, pl.ds((2 * x + h) * group, group)], p_local
    )
    own_out.start()

    chunks = gathered.shape[1]
    piece_rows = rows // chunks
    slab = 32 if piece_rows % 32 == 0 else 16 if piece_rows % 16 == 0 else 8
    per_chunk = piece_rows // slab

    @pl.loop(0, rows // slab)
    def _(r):
        values = tokens[pl.ds(r * slab, slab), :].astype(jnp.float32)
        center = jnp.mean(values, axis=-1, keepdims=True)
        moved = values - center
        spread = jnp.mean(moved * moved, axis=-1, keepdims=True)
        normed = moved * (1.0 / jnp.sqrt(spread + EPSILON))
        changed = normed * (1.0 + scale_mod[...]) + shift_mod[...]
        gathered[z, r // per_chunk, h, pl.ds((r % per_chunk) * slab, slab), :] = (
            changed.astype(jnp.bfloat16)
        )

    pl.semaphore_wait(barrier, 2 * nz + 1)

    for n in range(per_core):
        k = n + h * (per_core - 1 - 2 * n)
        target = h * per_core + k
        here, away = target == z, target != z
        local = jnp.logical_and(here, primary)
        beside = jnp.logical_and(here, other)
        for m, weight in enumerate((query_weight, key_weight, value_weight)):
            taken = pl.ds(pl.multiple_of(k * cols, cols), cols)
            whole = (pl.ds(z * depth, depth), pl.ds(m * cols, cols))
            piece = (pl.ds(z * depth + y * half, half), pl.ds(m * cols, cols))
            full_src = weight.at[:, taken]
            half_src = weight.at[pl.ds(y * half, half), taken]
            pl.when(local)(
                lambda src=full_src, index=whole, m=m: pltpu.make_async_copy(
                    src, weights.at[index], w_recv.at[z, m]
                ).start()
            )
            for cond, src, index in ((beside, full_src, whole), (away, half_src, piece)):
                post(
                    weights,
                    lambda index=index: index,
                    w_send.at[n, m],
                    w_recv.at[z, m],
                    {"outer": target, "head": x},
                    cond,
                    lambda src=src: src,
                )

    def shard(bt, c):
        return lambda: (bt, c, h)

    def near(t):
        start = b[t] * depth + (y * half if t else 0)
        return lambda: (pl.ds(start, half if t else depth), slice(None))

    def far(bt, m):
        return weights.at[pl.ds(bt * depth + (1 - y) * half, half), pl.ds(m * cols, cols)]

    b = [block(t) for t in range(nz)]
    def part(bt, gx, gy):
        start = (2 * gx + h) * group + gy * group_half
        return lambda: (bt, pl.ds(start, group_half))

    def out_source():
        return out_weight.at[pl.ds(y * group_half, group_half), :]

    def own_out_to(n, target, cond):
        post(
            out_full, part(z, x, y), o_own.at[n], o_recv.at[z], {"outer": target}, cond, out_source
        )

    def give_tokens():
        for c in range(chunks):
            post(gathered, shard(z, c), t_own.at[0, c], t_recv.at[z, c], {"outer": inner})
            post(gathered, shard(z, c), t_own.at[1, c], t_recv.at[z, c], {"outer": outer}, middle)
        own_out_to(0, inner, end)
        own_out_to(1, outer, middle)
        for c in range(chunks):
            post(gathered, shard(z, c), s_send.at[z, c], s_recv.at[z, c], sibling)

    for t in range(nz):
        for m in range(3):
            index = lambda t=t, m=m: (near(t)()[0], pl.ds(m * cols, cols))
            view = weights.at[index()]
            pl.when(primary)(lambda: arrive(view, w_recv.at[b[t], m]))
            post(weights, index, wx_send.at[t, m], wx_recv.at[t, m], across_x, primary)
            pl.when(other)(lambda: arrive(view, wx_recv.at[t, m]))
            if t:
                post(weights, index, wy_send.at[t, m], wy_recv.at[t, m], across_y)
        if t == 1:
            give_tokens()

    post(out_full, part(z, x, y), p_send.at[0], p_recv.at[0], across_x, None, out_source)
    own_index = lambda: (z, pl.ds((2 * x + h) * group, group))
    post(out_full, own_index, p_send.at[1], p_recv.at[1], sibling, None, lambda: out_weight)

    def take_tokens(t, cond=None):
        bt = b[t]
        moves = middle if cond is None else jnp.logical_and(middle, cond)
        target = inner if t == 1 else outer
        return [take_chunk(t, c, bt, cond, moves, target) for c in range(chunks)]

    def take_chunk(t, c, bt, cond, moves, target):
        view = lambda: gathered.at[shard(bt, c)()]

        def run():
            when(cond, lambda: arrive(view(), t_recv.at[bt, c]))
            pl.when(moves)(
                lambda: send(view, view, t_fwd.at[t, c], t_recv.at[bt, c], {"outer": target})
                and None
            )
            when(
                cond,
                lambda: send(view, view, s_send.at[bt, c], s_recv.at[bt, c], sibling) and None,
            )

        return run

    for one, two in zip(take_tokens(1), take_tokens(2, middle)):
        one()
        two()
    own_out_to(0, inner, middle)
    for t in range(1, nz):
        for m in range(3):
            arrive(far(b[t], m), wy_recv.at[t, m])

    def beside(bt, c):
        arrive(gathered.at[bt, c, 1 - h], s_recv.at[bt, c])

    def normed_head(projected, gain):
        square = jnp.mean(projected * projected, axis=-1, keepdims=True)
        return (projected * (1.0 / jnp.sqrt(square + EPSILON)) * gain).astype(jnp.bfloat16)

    def project(bt, before=()):
        def piece_of(c):
            piece = gathered[bt, c].reshape(2 * piece_rows, width)
            spot = pl.ds(pl.multiple_of(c * 2 * piece_rows, 2 * piece_rows), 2 * piece_rows)
            mine = pl.ds(pl.multiple_of(c * piece_rows, piece_rows), piece_rows)
            both = jnp.dot(
                piece, weights[:, : 2 * cols], preferred_element_type=jnp.float32
            )
            for i in range(heads):
                lo = i * head_dim
                query = normed_head(both[:, lo : lo + head_dim], query_gain[...])
                for core in range(2):
                    queries[i, bt, core, mine, :] = query[
                        core * piece_rows : (core + 1) * piece_rows
                    ]
                kv[0, i, x * nz + bt, spot, :] = normed_head(
                    both[:, cols + lo : cols + lo + head_dim], key_gain[...]
                )
            value = jnp.dot(
                piece, weights[:, 2 * cols :], preferred_element_type=jnp.float32
            ).astype(jnp.bfloat16)
            for i in range(heads):
                lo = i * head_dim
                kv[1, i, x * nz + bt, spot, :] = value[:, lo : lo + head_dim]
            view = lambda: kv.at[:, :, x * nz + bt, spot]
            send(view, view, kv_send.at[bt, c], kv_recv.at[bt, c], across_x)

        @pl.loop(0, chunks)
        def _(c):
            for n, step in enumerate(before):
                pl.when(c == n)(step)
            beside(bt, c)
            piece_of(c)

    def out_near(t, cond=None):
        bt = b[t]

        def run():
            mine = part(bt, x, y)
            arrive(out_full.at[mine()], o_recv.at[bt])
            target = inner if t == 1 else outer
            view = lambda: out_full.at[mine()]
            pl.when(middle)(
                lambda: send(view, view, o_fwd.at[t], o_recv.at[bt], {"outer": target}) and None
            )
            send(view, view, oy_send.at[t], oy_recv.at[t], across_y)
            send(view, view, ox_send.at[t], ox_recv.at[t], across_x)
            send(view, view, os_send.at[t, 0], os_recv.at[t, 0], sibling)

        when(cond, run)

    def out_second(t):
        bt = b[t]
        side, over = part(bt, x, 1 - y), part(bt, 1 - x, y)
        side_view, over_view = lambda: out_full.at[side()], lambda: out_full.at[over()]
        arrive(side_view(), oy_recv.at[t])
        if t == nz - 1:
            send(side_view, side_view, od_send.at[t], od_recv.at[t], across_x)
        send(side_view, side_view, os_send.at[t, 1], os_recv.at[t, 1], sibling)
        arrive(over_view(), ox_recv.at[t])
        if t < nz - 1:
            send(over_view, over_view, od_send.at[t], od_recv.at[t], across_y)
        send(over_view, over_view, os_send.at[t, 2], os_recv.at[t, 2], sibling)

    def out_third(t):
        last = part(b[t], 1 - x, 1 - y)
        view = lambda: out_full.at[last()]
        arrive(view(), od_recv.at[t])
        send(view, view, os_send.at[t, 3], os_recv.at[t, 3], sibling)

    project(b[0])
    project(b[1])
    out_near(1)
    crossed = part(z, 1 - x, y)
    arrive(out_full.at[crossed()], p_recv.at[0])
    post(out_full, crossed, od_send.at[0], od_recv.at[0], across_y)
    post(out_full, crossed, os_send.at[0, 2], os_recv.at[0, 2], sibling)
    project(b[2], take_tokens(2, end))
    project(b[3], take_tokens(3))
    out_near(2, middle)
    out_near(3, middle)
    out_second(1)
    out_third(0)
    for t in range(nz):
        for c in range(chunks):
            spot = pl.ds(c * 2 * piece_rows, 2 * piece_rows)
            arrive(kv.at[:, :, (1 - x) * nz + b[t], spot], kv_recv.at[b[t], c])

    factor = math.log2(math.e) / math.sqrt(head_dim)
    key_blocks, key_rows = kv.shape[2], kv.shape[3]
    span = 2 if key_blocks % 2 == 0 else 1

    def attend_rows(query, i):
        def score(c):
            keys = kv[0, i, c : c + span].reshape(span * key_rows, head_dim)
            return lax.dot_general(
                query, keys, (((1,), (1,)), ((), ())), preferred_element_type=jnp.float32
            )

        total = result = top = None
        scores = score(0)
        for c in range(0, key_blocks, span):
            after = score(c + span) if c + span < key_blocks else None
            values = kv[1, i, c : c + span].reshape(span * key_rows, head_dim)
            peak = jnp.max(scores, axis=-1, keepdims=True)
            if c:
                peak = jnp.maximum(top, peak)
            probs = jnp.exp2((scores - peak) * factor)
            fresh = jnp.sum(probs, axis=-1, keepdims=True)
            gained = jnp.dot(
                probs.astype(jnp.bfloat16), values, preferred_element_type=jnp.float32
            )
            if c:
                shrink = jnp.exp2((top - peak) * factor)
                total, result = total * shrink + fresh, result * shrink + gained
            else:
                total, result = fresh, gained
            top, scores = peak, after
        return (result / total).astype(jnp.bfloat16)

    def place():
        return (slice(None), pl.ds((h * nz + z) * cols, cols))

    duties = {
        0: lambda: (out_near(2, end), out_third(1)),
        1: lambda: out_near(3, end),
        2: lambda: out_second(2),
        3: lambda: out_second(3),
    }

    @pl.loop(0, nz)
    def _(j):
        for at, duty in duties.items():
            pl.when(j == at)(lambda duty=duty: duty() and None)
        bt = block(nz - 1 - j)

        @pl.loop(0, heads)
        def _(i):
            query = queries[i, bt].reshape(2 * rows, head_dim)
            spot = pl.ds(pl.multiple_of(i * head_dim, head_dim), head_dim)
            staged[bt, :, :, spot] = attend_rows(query, i).reshape(2, rows, head_dim)

        for core in range(2):
            self_place = jnp.logical_and(bt == z, h == core)

            def keep():
                mixed[place()] = staged[bt, core]

            def give():
                send(
                    lambda: staged.at[bt, core],
                    lambda: mixed.at[place()],
                    m_send.at[bt, core],
                    m_recv.at[h * nz + z],
                    {"outer": bt, "head": core},
                )

            pl.when(self_place)(keep)
            pl.when(jnp.logical_not(self_place))(give)

    out_third(2)
    out_third(3)
    for zs in range(nz):
        for hs in range(2):
            k = hs * nz + zs
            pl.when(jnp.logical_or(z != zs, h != hs))(
                lambda k=k: arrive(mixed.at[:, k * cols : (k + 1) * cols], m_recv.at[k])
            )

    def sibling_part(bt, gx, gy):
        start = (2 * gx + 1 - h) * group + gy * group_half
        return out_full.at[bt, pl.ds(start, group_half)]

    own_out.wait()
    arrive(out_full.at[z, pl.ds((2 * x + 1 - h) * group, group)], p_recv.at[1])

    for t in range(nz):
        bt = b[t]
        for n, (gx, gy) in enumerate(((x, y), (x, 1 - y), (1 - x, y), (1 - x, 1 - y))):
            if t or n > 1:
                arrive(sibling_part(bt, gx, gy), os_recv.at[t, n])
        summed = jnp.zeros((rows, block_cols), jnp.float32)
        for g in range(4):
            term = jnp.dot(
                mixed[:, g * group : (g + 1) * group],
                out_full[bt, g * group : (g + 1) * group, :],
                preferred_element_type=jnp.float32,
            )
            summed = summed + term.astype(jnp.bfloat16).astype(jnp.float32)
        here = pl.ds(pl.multiple_of(bt * block_cols, block_cols), block_cols)
        out[:, here] = (summed * gate_mod[:, here]).astype(jnp.bfloat16)

    for cond, made in sends:
        when(cond, lambda made=made: made().wait_send())

    def sent(view, sem):
        pltpu.make_async_copy(view, view, sem).wait()

    for t in range(nz):
        bt = b[t]
        piece = out_full.at[part(bt, x, y)()]
        for c in range(chunks):
            tok = gathered.at[shard(bt, c)()]
            spot = pl.ds(c * 2 * piece_rows, 2 * piece_rows)
            sent(kv.at[:, :, x * nz + bt, spot], kv_send.at[bt, c])
            if t:
                pl.when(middle)(lambda tok=tok, t=t, c=c: sent(tok, t_fwd.at[t, c]))
                sent(tok, s_send.at[bt, c])
        if t:
            pl.when(middle)(lambda piece=piece, t=t: sent(piece, o_fwd.at[t]))
            sent(piece, oy_send.at[t])
            sent(piece, ox_send.at[t])
            sent(piece, od_send.at[t])
        for n in range(4):
            if t or n > 2:
                sent(piece, os_send.at[t, n])
    for zs in range(nz):
        for hs in range(2):
            pl.when(jnp.logical_or(z != zs, h != hs))(
                lambda zs=zs, hs=hs: sent(staged.at[zs, hs], m_send.at[zs, hs])
            )


def fused(nz, tokens, shift_mod, scale_mod, gate_mod, *rest):
    wq, wk, wv, wo, query_gain, key_gain = rest
    _, rows, width = tokens.shape
    head_dim = query_gain.shape[0]
    depth, group_cols = wq.shape
    heads = 4 * group_cols // head_dim // (2 * nz)
    cols = heads * head_dim
    chunks = 2
    dma = lambda *shape: pltpu.SemaphoreType.DMA(shape)
    vmem = pl.BlockSpec(memory_space=pltpu.VMEM)
    anywhere = pl.BlockSpec(memory_space=pl.ANY)
    result = pl.pallas_call(
        functools.partial(sublayer, nz, head_dim),
        out_shape=jax.ShapeDtypeStruct((rows, width), jnp.bfloat16),
        in_specs=[vmem] * 6 + [anywhere] * 4,
        out_specs=vmem,
        scratch_shapes=[
            pltpu.VMEM((width, 3 * cols), jnp.bfloat16),
            pltpu.VMEM((nz, chunks, 2, rows // chunks, width), jnp.bfloat16),
            pltpu.VMEM((heads, nz, 2, rows, head_dim), jnp.bfloat16),
            pltpu.VMEM((2, heads, 2 * nz, 2 * rows, head_dim), jnp.bfloat16),
            pltpu.VMEM((nz, 4 * wo.shape[0], wo.shape[1]), jnp.bfloat16),
            pltpu.VMEM((rows, width), jnp.bfloat16),
            pltpu.VMEM((nz, 2, rows, cols), jnp.bfloat16),
            dma(nz // 2, 3),
            dma(nz, 3),
            dma(nz, 3),
            dma(nz, 3),
            dma(nz, 3),
            dma(nz, 3),
            dma(2, chunks),
            dma(nz, chunks),
            dma(nz, chunks),
            dma(nz, chunks),
            dma(nz, chunks),
            dma(nz, chunks),
            dma(nz, chunks),
            dma(nz, 2),
            dma(2 * nz),
            pltpu.SemaphoreType.DMA,
            dma(2),
            dma(2),
            dma(2),
            dma(nz),
            dma(nz),
            dma(nz),
            dma(nz),
            dma(nz),
            dma(nz),
            dma(nz),
            dma(nz),
            dma(nz, 4),
            dma(nz, 4),
        ],
        compiler_params=pltpu.CompilerParams(
            collective_id=0, has_side_effects=True, vmem_limit_bytes=67043328
        ),
        name="sublayer",
    )(
        tokens[0],
        shift_mod,
        scale_mod,
        gate_mod,
        query_gain[None],
        key_gain[None],
        wq,
        wk,
        wv,
        wo,
    )
    return result[None]


def fits(mesh, args):
    sizes = mesh.shape
    head_dim, (depth, group_cols) = args[8].shape[0], args[4].shape
    nz = sizes["outer"]
    return (
        sizes["inner"] == 2
        and sizes["head"] == 2
        and sizes["clip"] == 2
        and nz == 4
        and args[0].shape[0] == 1
        and args[0].shape[1] % 32 == 0
        and head_dim % 128 == 0
        and (4 * group_cols) % (2 * nz * head_dim) == 0
        and depth % 32 == 0
    )


def solution(mesh):
    in_specs = (
        P("clip", ("outer", "inner", "head"), None),
        P("clip", None),
        P("clip", None),
        P("clip", None),
        P("outer", ("inner", "head")),
        P("outer", ("inner", "head")),
        P("outer", ("inner", "head")),
        P(("inner", "head"), "outer"),
        P(),
        P(),
    )
    out_specs = P("clip", ("outer", "inner", "head"), None)

    def body(*args):
        if fits(mesh, args):
            return fused(mesh.shape["outer"], *args)
        return per_device(*args)

    return jax.shard_map(
        body, mesh=mesh, in_specs=in_specs, out_specs=out_specs, check_vma=False
    )
```

```python
import functools
import math

import jax
import jax.numpy as jnp
from jax import lax
from jax.experimental import pallas as pl
from jax.experimental.pallas import tpu as pltpu
from jax.sharding import PartitionSpec as P

EPSILON = 1e-06


def modulate(tokens, shift_mod, scale_mod):
    values = tokens.astype(jnp.float32)
    center = jnp.mean(values, axis=-1, keepdims=True)
    spread = jnp.mean(jnp.square(values - center), axis=-1, keepdims=True)
    normed = (values - center) / jnp.sqrt(spread + EPSILON)
    return (normed * (1.0 + scale_mod[:, None, :]) + shift_mod[:, None, :]).astype(jnp.bfloat16)


def head_norm(projected, gain_vec, head_dim):
    shaped = projected.reshape(projected.shape[:-1] + (projected.shape[-1] // head_dim, head_dim))
    mean_square = jnp.mean(jnp.square(shaped), axis=-1, keepdims=True)
    return (shaped / jnp.sqrt(mean_square + EPSILON) * gain_vec).astype(jnp.bfloat16)


def per_device(
    tokens,
    shift_mod,
    scale_mod,
    gate_mod,
    query_weight,
    key_weight,
    value_weight,
    out_weight,
    query_gain,
    key_gain,
):
    head_dim = query_gain.shape[0]
    modulated = modulate(tokens, shift_mod, scale_mod)
    gathered = lax.all_gather(modulated, ("inner", "head"), axis=1, tiled=True)
    clip_count, row_count, model_width = gathered.shape
    flattened = gathered.reshape(clip_count * row_count, model_width)
    local_cols = query_weight.shape[1]
    head_count = local_cols // head_dim
    full_query, full_key, full_value = (
        lax.all_gather(query_weight, "outer", axis=0, tiled=True),
        lax.all_gather(key_weight, "outer", axis=0, tiled=True),
        lax.all_gather(value_weight, "outer", axis=0, tiled=True),
    )
    query_proj = jnp.dot(flattened, full_query, preferred_element_type=jnp.float32)
    key_proj = jnp.dot(flattened, full_key, preferred_element_type=jnp.float32)
    value_proj = jnp.dot(flattened, full_value, preferred_element_type=jnp.float32)
    query_heads = head_norm(
        query_proj.reshape(clip_count, row_count, local_cols), query_gain, head_dim
    )
    key_send = head_norm(key_proj.reshape(clip_count, row_count, local_cols), key_gain, head_dim)
    key_send = key_send.reshape(clip_count, row_count, local_cols)
    value_send = value_proj.astype(jnp.bfloat16).reshape(clip_count, row_count, local_cols)
    root_size = math.sqrt(head_dim)
    full_out = lax.all_gather(out_weight, "outer", axis=1, tiled=True)
    running_max = jnp.full((clip_count, head_count, row_count), -1e30, jnp.float32)
    key_piece = lax.all_gather(key_send, "outer", axis=1, tiled=True)
    value_piece = lax.all_gather(value_send, "outer", axis=1, tiled=True)
    key_count = key_piece.shape[1]
    key_piece = key_piece.reshape(clip_count, key_count, head_count, head_dim)
    value_piece = value_piece.reshape(clip_count, key_count, head_count, head_dim)
    scores = (
        jnp.einsum("cqhd,ckhd->chqk", query_heads, key_piece, preferred_element_type=jnp.float32)
        / root_size
    )
    new_max = jnp.maximum(running_max, jnp.max(scores, axis=-1))
    weights = jnp.exp(scores - new_max[..., None])
    new_sum = jnp.sum(weights, axis=-1)
    new_acc = jnp.einsum(
        "chqk,ckhd->chqd",
        weights.astype(jnp.bfloat16),
        value_piece,
        preferred_element_type=jnp.float32,
    )
    head_out = new_acc / new_sum[..., None]
    mixed = (
        jnp.transpose(head_out, (0, 2, 1, 3))
        .reshape(clip_count * row_count, local_cols)
        .astype(jnp.bfloat16)
    )
    partial_value = jnp.dot(mixed, full_out, preferred_element_type=jnp.float32).reshape(
        clip_count, row_count, -1
    )
    summed = lax.psum_scatter(
        partial_value.astype(jnp.bfloat16), ("inner", "head"), scatter_dimension=1, tiled=True
    ).astype(jnp.float32)
    return (summed * gate_mod[:, None, :]).astype(jnp.bfloat16)


def sublayer(
    nz,
    head_dim,
    tokens,
    shift_mod,
    scale_mod,
    gate_mod,
    query_gain,
    key_gain,
    query_weight,
    key_weight,
    value_weight,
    out_weight,
    out,
    weights,
    gathered,
    queries,
    kv,
    out_full,
    mixed,
    state,
    w_send,
    w_recv,
    wx_send,
    wx_recv,
    wy_send,
    wy_recv,
    t_own,
    t_fwd,
    t_recv,
    s_send,
    s_recv,
    kv_send,
    kv_recv,
    m_send,
    m_recv,
    p_local,
    p_send,
    p_recv,
    o_own,
    o_fwd,
    o_recv,
    oy_send,
    oy_recv,
    ox_send,
    ox_recv,
    od_send,
    od_recv,
    os_send,
    os_recv,
    fetched,
):
    y, z = lax.axis_index("clip"), lax.axis_index("outer")
    x, h = lax.axis_index("inner"), lax.axis_index("head")
    rows, width = tokens.shape
    depth = query_weight.shape[0]
    half = depth // 2
    cols = queries.shape[0] * head_dim
    heads = queries.shape[0]
    per_core = nz // 2
    group, block_cols = out_weight.shape
    group_half = group // 2
    high = z // (nz // 2)
    inner, outer = z + 1 - 2 * high, z - 1 + 2 * high
    middle = jnp.logical_and(z > 0, z < nz - 1)
    end = jnp.logical_not(middle)
    primary = h == x
    other = jnp.logical_not(primary)

    sibling, across_y, across_x = {"head": 1 - h}, {"clip": 1 - y}, {"inner": 1 - x}
    sends = []

    def block(t):
        first, odd = 1 - t // 2, t % 2
        return (
            first * (1 - odd) * z
            + first * odd * (1 - z + 4 * high)
            + (1 - first) * ((1 - high) * t + high * (3 - t))
        )

    def when(cond, run):
        if cond is None:
            run()
        else:
            pl.when(cond)(run)

    def send(src, dst, send_sem, recv_sem, device, cond=None):
        def make():
            return pltpu.make_async_remote_copy(
                src_ref=src(),
                dst_ref=dst(),
                send_sem=send_sem,
                recv_sem=recv_sem,
                device_id=device,
                device_id_type=pl.DeviceIdType.MESH,
            )

        when(cond, lambda: make().start())
        return make

    def post(ref, index, send_sem, recv_sem, device, cond=None, source=None):
        dst = lambda: ref.at[index()]
        src = dst if source is None else source
        made = send(src, dst, send_sem, recv_sem, device, cond)
        sends.append((cond, made))

    def arrive(view, sem):
        pltpu.make_async_copy(view, view, sem).wait()

    fetch = pltpu.make_async_copy(tokens, out, fetched)
    fetch.start()

    barrier = pltpu.get_barrier_semaphore()

    def greet(device):
        pl.semaphore_signal(
            barrier, inc=1, device_id=device, device_id_type=pl.DeviceIdType.MESH
        )

    for zs in range(nz):
        for hs in range(2):
            away = jnp.logical_or(z != zs, h != hs)
            pl.when(away)(lambda zs=zs, hs=hs: greet({"outer": zs, "head": hs}))
    greet(across_y)
    greet(across_x)
    pl.semaphore_wait(barrier, 2 * nz + 1)

    for n in range(per_core):
        k = n + h * (per_core - 1 - 2 * n)
        target = h * per_core + k
        here, away = target == z, target != z
        local = jnp.logical_and(here, primary)
        beside = jnp.logical_and(here, other)
        for m, weight in enumerate((query_weight, key_weight, value_weight)):
            taken = pl.ds(pl.multiple_of(k * cols, cols), cols)
            whole = (pl.ds(z * depth, depth), pl.ds(m * cols, cols))
            piece = (pl.ds(z * depth + y * half, half), pl.ds(m * cols, cols))
            full_src = weight.at[:, taken]
            half_src = weight.at[pl.ds(y * half, half), taken]
            pl.when(local)(
                lambda src=full_src, index=whole, m=m: pltpu.make_async_copy(
                    src, weights.at[index], w_recv.at[z, m]
                ).start()
            )
            for cond, src, index in ((beside, full_src, whole), (away, half_src, piece)):
                post(
                    weights,
                    lambda index=index: index,
                    w_send.at[n, m],
                    w_recv.at[z, m],
                    {"outer": target, "head": x},
                    cond,
                    lambda src=src: src,
                )

    own_out = pltpu.make_async_copy(
        out_weight, out_full.at[z, pl.ds((2 * x + h) * group, group)], p_local
    )
    own_out.start()

    fetch.wait()
    chunks = gathered.shape[1]
    piece_rows = rows // chunks
    slab = 32 if piece_rows % 32 == 0 else 16 if piece_rows % 16 == 0 else 8
    per_chunk = piece_rows // slab

    @pl.loop(0, rows // slab)
    def _(r):
        values = out[pl.ds(r * slab, slab), :].astype(jnp.float32)
        center = jnp.mean(values, axis=-1, keepdims=True)
        moved = values - center
        spread = jnp.mean(moved * moved, axis=-1, keepdims=True)
        normed = moved * (1.0 / jnp.sqrt(spread + EPSILON))
        changed = normed * (1.0 + scale_mod[...]) + shift_mod[...]
        gathered[z, r // per_chunk, h, pl.ds((r % per_chunk) * slab, slab), :] = (
            changed.astype(jnp.bfloat16)
        )

    def shard(bt, c):
        return lambda: (bt, c, h)

    def near(t):
        start = b[t] * depth + (y * half if t else 0)
        return lambda: (pl.ds(start, half if t else depth), slice(None))

    def far(bt, m):
        return weights.at[pl.ds(bt * depth + (1 - y) * half, half), pl.ds(m * cols, cols)]

    b = [block(t) for t in range(nz)]
    def part(bt, gx, gy):
        start = (2 * gx + h) * group + gy * group_half
        return lambda: (bt, pl.ds(start, group_half))

    def quarter(bt, gx, gy, c):
        size = group_half // 2
        start = (2 * gx + h) * group + gy * group_half + c * size
        return lambda: (bt, pl.ds(start, size))

    def out_source():
        return out_weight.at[pl.ds(y * group_half, group_half), :]

    def own_out_to(n, target, cond):
        for c in range(2):
            size = group_half // 2
            source = out_weight.at[pl.ds(y * group_half + c * size, size), :]
            post(
                out_full,
                quarter(z, x, y, c),
                o_own.at[n, c],
                o_recv.at[z, c],
                {"outer": target},
                cond,
                lambda source=source: source,
            )

    def give_tokens():
        for c in range(chunks):
            post(gathered, shard(z, c), t_own.at[0, c], t_recv.at[z, c], {"outer": inner})
            post(gathered, shard(z, c), t_own.at[1, c], t_recv.at[z, c], {"outer": outer}, middle)
        own_out_to(0, inner, end)
        own_out_to(1, outer, middle)
        for c in range(chunks):
            post(gathered, shard(z, c), s_send.at[z, c], s_recv.at[z, c], sibling)

    for t in range(nz):
        for m in range(3):
            index = lambda t=t, m=m: (near(t)()[0], pl.ds(m * cols, cols))
            view = weights.at[index()]
            pl.when(primary)(lambda: arrive(view, w_recv.at[b[t], m]))
            post(weights, index, wx_send.at[t, m], wx_recv.at[t, m], across_x, primary)
            pl.when(other)(lambda: arrive(view, wx_recv.at[t, m]))
            if t:
                post(weights, index, wy_send.at[t, m], wy_recv.at[t, m], across_y)
        if t == 1:
            give_tokens()

    post(out_full, part(z, x, y), p_send.at[0], p_recv.at[0], across_x, None, out_source)
    own_index = lambda: (z, pl.ds((2 * x + h) * group, group))
    post(out_full, own_index, p_send.at[1], p_recv.at[1], sibling, None, lambda: out_weight)

    def take_tokens(t, cond=None):
        bt = b[t]
        moves = middle if cond is None else jnp.logical_and(middle, cond)
        target = inner if t == 1 else outer
        return [take_chunk(t, c, bt, cond, moves, target) for c in range(chunks)]

    def take_chunk(t, c, bt, cond, moves, target):
        view = lambda: gathered.at[shard(bt, c)()]

        def run():
            when(cond, lambda: arrive(view(), t_recv.at[bt, c]))
            pl.when(moves)(
                lambda: send(view, view, t_fwd.at[t, c], t_recv.at[bt, c], {"outer": target})
                and None
            )
            when(
                cond,
                lambda: send(view, view, s_send.at[bt, c], s_recv.at[bt, c], sibling) and None,
            )

        return run

    for one, two in zip(take_tokens(1), take_tokens(2, middle)):
        one()
        two()
    own_out_to(0, inner, middle)
    for t in range(1, nz):
        for m in range(3):
            arrive(far(b[t], m), wy_recv.at[t, m])

    def beside(bt, c):
        arrive(gathered.at[bt, c, 1 - h], s_recv.at[bt, c])

    def normed_head(projected, gain):
        square = jnp.mean(projected * projected, axis=-1, keepdims=True)
        return (projected * (1.0 / jnp.sqrt(square + EPSILON)) * gain).astype(jnp.bfloat16)

    def project(bt, before=()):
        def piece_of(c):
            piece = gathered[bt, c].reshape(2 * piece_rows, width)
            spot = pl.ds(pl.multiple_of(c * 2 * piece_rows, 2 * piece_rows), 2 * piece_rows)
            mine = pl.ds(pl.multiple_of(c * piece_rows, piece_rows), piece_rows)
            both = jnp.dot(
                piece, weights[:, : 2 * cols], preferred_element_type=jnp.float32
            )
            for i in range(heads):
                lo = i * head_dim
                query = normed_head(both[:, lo : lo + head_dim], query_gain[...])
                for core in range(2):
                    queries[i, bt, core, mine, :] = query[
                        core * piece_rows : (core + 1) * piece_rows
                    ]
                kv[0, i, 2 * bt + x, spot, :] = normed_head(
                    both[:, cols + lo : cols + lo + head_dim], key_gain[...]
                )
            value = jnp.dot(
                piece, weights[:, 2 * cols :], preferred_element_type=jnp.float32
            ).astype(jnp.bfloat16)
            for i in range(heads):
                lo = i * head_dim
                kv[1, i, 2 * bt + x, spot, :] = value[:, lo : lo + head_dim]
            view = lambda: kv.at[:, :, 2 * bt + x, spot]
            send(view, view, kv_send.at[bt, c], kv_recv.at[bt, c], across_x)

        @pl.loop(0, chunks)
        def _(c):
            for n, step in enumerate(before):
                pl.when(c == n)(step)
            beside(bt, c)
            piece_of(c)

    def out_near(t, cond=None, pieces=(0, 1)):
        bt = b[t]

        def run():
            for c in pieces:
                mine = quarter(bt, x, y, c)
                view = lambda: out_full.at[mine()]
                arrive(view(), o_recv.at[bt, c])
                target = inner if t == 1 else outer
                pl.when(middle)(
                    lambda: send(view, view, o_fwd.at[t, c], o_recv.at[bt, c], {"outer": target})
                    and None
                )
                send(view, view, oy_send.at[t, c], oy_recv.at[t, c], across_y)
                send(view, view, ox_send.at[t, c], ox_recv.at[t, c], across_x)
                send(view, view, os_send.at[t, c], os_recv.at[t, c], sibling)

        when(cond, run)

    def out_second(t, pieces=(0, 1)):
        bt = b[t]
        for c in pieces:
            side, over = quarter(bt, x, 1 - y, c), quarter(bt, 1 - x, y, c)
            side_view, over_view = lambda: out_full.at[side()], lambda: out_full.at[over()]
            arrive(side_view(), oy_recv.at[t, c])
            if t > 1 and c:
                send(side_view, side_view, od_send.at[t, c], od_recv.at[t, c], across_x)
            send(side_view, side_view, os_send.at[t, 2 + c], os_recv.at[t, 2 + c], sibling)
            arrive(over_view(), ox_recv.at[t, c])
            if t == 1 or not c:
                send(over_view, over_view, od_send.at[t, c], od_recv.at[t, c], across_y)
            send(over_view, over_view, os_send.at[t, 4 + c], os_recv.at[t, 4 + c], sibling)

    def out_third(t):
        if t == 0:
            last = part(z, 1 - x, 1 - y)
            view = lambda: out_full.at[last()]
            arrive(view(), od_recv.at[0, 0])
            send(view, view, os_send.at[0, 1], os_recv.at[0, 1], sibling)
            return
        for c in range(2):
            last = quarter(b[t], 1 - x, 1 - y, c)
            view = lambda: out_full.at[last()]
            arrive(view(), od_recv.at[t, c])
            send(view, view, os_send.at[t, 6 + c], os_recv.at[t, 6 + c], sibling)

    factor = math.log2(math.e) / math.sqrt(head_dim)
    key_rows = kv.shape[3]

    def score(query, i, bt):
        keys = kv[0, i, pl.ds(2 * bt, 2)].reshape(2 * key_rows, head_dim)
        return lax.dot_general(
            query, keys, (((1,), (1,)), ((), ())), preferred_element_type=jnp.float32
        )

    def wide(column, times):
        return jnp.concatenate([column] * times, axis=1)

    def fold(carry, scores, i, bt):
        values = kv[1, i, pl.ds(2 * bt, 2)].reshape(2 * key_rows, head_dim)
        shape = (scores.shape[0], head_dim)
        peak = jnp.broadcast_to(jnp.max(scores, axis=-1, keepdims=True), shape)
        if carry is not None:
            top, total, result = carry
            peak = jnp.maximum(top, peak)
        times = scores.shape[1] // head_dim
        probs = jnp.exp2((scores - wide(peak, times)) * factor)
        fresh = jnp.broadcast_to(jnp.sum(probs, axis=-1, keepdims=True), shape)
        gained = jnp.dot(
            probs.astype(jnp.bfloat16), values, preferred_element_type=jnp.float32
        )
        if carry is None:
            return peak, fresh, gained
        shrink = jnp.exp2((top - peak) * factor)
        return peak, total * shrink + fresh, result * shrink + gained

    def query_of(i, bt):
        return queries[i, bt].reshape(2 * rows, head_dim)

    def keep_state(u, i, carry):
        for n, value in enumerate(carry):
            state[n, u, i] = value

    def load_state(u, i):
        return [state[n, u, i] for n in range(3)]

    def finish(i, bt, carry):
        _, total, result = carry
        queries[i, bt] = (result / total).astype(jnp.bfloat16).reshape(2, rows, head_dim)

    def first_pass(t, bt, done, duty=None):
        @pl.loop(0, heads)
        def _(i):
            if duty is not None:
                duty(i)
            query = query_of(i, bt)
            carry, scores = None, score(query, i, b[0])
            for n in range(t + 1):
                after = score(query, i, b[n + 1]) if n < t else None
                carry = fold(carry, scores, i, b[n])
                scores = after
            done(i, carry)

    def later_pass(u, bt, bk):
        carried = [load_state(u, i) for i in range(heads)]
        scores = score(query_of(0, bt), 0, bk)
        ends = []
        for i in range(heads):
            after = score(query_of(i + 1, bt), i + 1, bk) if i + 1 < heads else None
            ends.append(fold(carried[i], scores, i, bk))
            scores = after
        for i in range(heads):
            finish(i, bt, ends[i])

    def keys_arrive(t):
        for c in range(chunks):
            spot = pl.ds(c * 2 * piece_rows, 2 * piece_rows)
            arrive(kv.at[:, :, 2 * b[t] + 1 - x, spot], kv_recv.at[b[t], c])

    def ahead():
        for t in range(nz - 1):
            keys_arrive(t)

        @pl.loop(0, 2)
        def _(u):
            pl.when(u == 1)(lambda: out_near(2, end, (0,)))
            first_pass(nz - 2, block(u + 1), lambda i, carry: keep_state(u, i, carry))

    def place(i):
        start = (h * nz + z) * cols + i * head_dim
        return (slice(None), pl.ds(pl.multiple_of(start, head_dim), head_dim))

    def hand_over(bt):
        for core in range(2):
            self_place = jnp.logical_and(bt == z, h == core)

            def keep():
                for i in range(heads):
                    mixed[place(i)] = queries[i, bt, core]

            def give():
                for i in range(heads):
                    send(
                        lambda: queries.at[i, bt, core],
                        lambda: mixed.at[place(i)],
                        m_send.at[bt, core],
                        m_recv.at[h * nz + z],
                        {"outer": bt, "head": core},
                    )

            pl.when(self_place)(keep)
            pl.when(jnp.logical_not(self_place))(give)

    project(b[0])
    project(b[1])
    out_near(1)
    crossed = part(z, 1 - x, y)
    arrive(out_full.at[crossed()], p_recv.at[0])
    post(out_full, crossed, od_send.at[0, 0], od_recv.at[0, 0], across_y)
    post(out_full, crossed, os_send.at[0, 0], os_recv.at[0, 0], sibling)
    project(b[2], take_tokens(2, end))
    project(b[3], take_tokens(3))
    out_near(2, middle)
    out_near(3, middle)
    out_second(1)
    out_third(0)
    ahead()
    out_near(2, end, (1,))
    keys_arrive(3)
    later_pass(0, b[1], b[3])
    hand_over(b[1])
    later_pass(1, b[2], b[3])
    hand_over(b[2])
    out_third(1)
    soon = min(1, heads - 1)
    first_pass(
        3,
        b[3],
        lambda i, carry: finish(i, b[3], carry),
        lambda i: pl.when(i == soon)(lambda: out_near(3, end, (0,))),
    )
    hand_over(b[3])
    out_near(3, end, (1,))
    first_pass(
        3,
        b[0],
        lambda i, carry: finish(i, b[0], carry),
        lambda i: pl.when(i == soon)(lambda: out_second(2)),
    )
    hand_over(b[0])
    out_second(3)
    out_third(2)
    for zs in range(nz):
        for hs in range(2):
            k = hs * nz + zs
            pl.when(jnp.logical_or(z != zs, h != hs))(
                lambda k=k: arrive(mixed.at[:, k * cols : (k + 1) * cols], m_recv.at[k])
            )

    def sibling_part(bt, gx, gy, c):
        size = group_half if c is None else group_half // 2
        start = (2 * gx + 1 - h) * group + gy * group_half + (c or 0) * size
        return out_full.at[bt, pl.ds(start, size)]

    own_out.wait()
    arrive(out_full.at[z, pl.ds((2 * x + 1 - h) * group, group)], p_recv.at[1])

    for t in range(nz):
        bt = b[t]
        if t == nz - 2:
            out_third(nz - 1)
        if t:
            for n, (gx, gy) in enumerate(((x, y), (x, 1 - y), (1 - x, y), (1 - x, 1 - y))):
                for c in range(2):
                    arrive(sibling_part(bt, gx, gy, c), os_recv.at[t, 2 * n + c])
        else:
            for n in range(2):
                arrive(sibling_part(z, 1 - x, y + n - 2 * n * y, None), os_recv.at[0, n])
        summed = jnp.zeros((rows, block_cols), jnp.float32)
        for g in range(4):
            term = jnp.dot(
                mixed[:, g * group : (g + 1) * group],
                out_full[bt, g * group : (g + 1) * group, :],
                preferred_element_type=jnp.float32,
            )
            summed = summed + term.astype(jnp.bfloat16).astype(jnp.float32)
        here = pl.ds(pl.multiple_of(bt * block_cols, block_cols), block_cols)
        out[:, here] = (summed * gate_mod[:, here]).astype(jnp.bfloat16)

    for cond, made in sends:
        when(cond, lambda made=made: made().wait_send())

    def sent(view, sem):
        pltpu.make_async_copy(view, view, sem).wait()

    for t in range(nz):
        bt = b[t]
        piece = out_full.at[quarter(bt, x, y, 0)()]
        for c in range(chunks):
            tok = gathered.at[shard(bt, c)()]
            spot = pl.ds(c * 2 * piece_rows, 2 * piece_rows)
            sent(kv.at[:, :, 2 * bt + x, spot], kv_send.at[bt, c])
            if t:
                pl.when(middle)(lambda tok=tok, t=t, c=c: sent(tok, t_fwd.at[t, c]))
                sent(tok, s_send.at[bt, c])
        if t:
            for c in range(2):
                pl.when(middle)(lambda piece=piece, t=t, c=c: sent(piece, o_fwd.at[t, c]))
                sent(piece, oy_send.at[t, c])
                sent(piece, ox_send.at[t, c])
                sent(piece, od_send.at[t, c])
            for n in range(8):
                sent(piece, os_send.at[t, n])
    sent(out_full.at[part(z, x, y)()], os_send.at[0, 1])
    for zs in range(nz):
        for hs in range(2):
            pl.when(jnp.logical_or(z != zs, h != hs))(
                lambda zs=zs, hs=hs: sent(queries.at[:, zs, hs], m_send.at[zs, hs])
            )


def fused(nz, tokens, shift_mod, scale_mod, gate_mod, *rest):
    wq, wk, wv, wo, query_gain, key_gain = rest
    _, rows, width = tokens.shape
    head_dim = query_gain.shape[0]
    depth, group_cols = wq.shape
    heads = 4 * group_cols // head_dim // (2 * nz)
    cols = heads * head_dim
    chunks = 2
    dma = lambda *shape: pltpu.SemaphoreType.DMA(shape)
    vmem = pl.BlockSpec(memory_space=pltpu.VMEM)
    anywhere = pl.BlockSpec(memory_space=pl.ANY)
    result = pl.pallas_call(
        functools.partial(sublayer, nz, head_dim),
        out_shape=jax.ShapeDtypeStruct((rows, width), jnp.bfloat16),
        in_specs=[anywhere] + [vmem] * 5 + [anywhere] * 4,
        out_specs=vmem,
        scratch_shapes=[
            pltpu.VMEM((width, 3 * cols), jnp.bfloat16),
            pltpu.VMEM((nz, chunks, 2, rows // chunks, width), jnp.bfloat16),
            pltpu.VMEM((heads, nz, 2, rows, head_dim), jnp.bfloat16),
            pltpu.VMEM((2, heads, 2 * nz, 2 * rows, head_dim), jnp.bfloat16),
            pltpu.VMEM((nz, 4 * wo.shape[0], wo.shape[1]), jnp.bfloat16),
            pltpu.VMEM((rows, width), jnp.bfloat16),
            pltpu.VMEM((3, 2, heads, 2 * rows, head_dim), jnp.float32),
            dma(nz // 2, 3),
            dma(nz, 3),
            dma(nz, 3),
            dma(nz, 3),
            dma(nz, 3),
            dma(nz, 3),
            dma(2, chunks),
            dma(nz, chunks),
            dma(nz, chunks),
            dma(nz, chunks),
            dma(nz, chunks),
            dma(nz, chunks),
            dma(nz, chunks),
            dma(nz, 2),
            dma(2 * nz),
            pltpu.SemaphoreType.DMA,
            dma(2),
            dma(2),
            dma(2, 2),
            dma(nz, 2),
            dma(nz, 2),
            dma(nz, 2),
            dma(nz, 2),
            dma(nz, 2),
            dma(nz, 2),
            dma(nz, 2),
            dma(nz, 2),
            dma(nz, 8),
            dma(nz, 8),
            pltpu.SemaphoreType.DMA,
        ],
        compiler_params=pltpu.CompilerParams(
            collective_id=0, has_side_effects=True, vmem_limit_bytes=67043328
        ),
        name="sublayer",
    )(
        tokens[0],
        shift_mod,
        scale_mod,
        gate_mod,
        query_gain[None],
        key_gain[None],
        wq,
        wk,
        wv,
        wo,
    )
    return result[None]


def fits(mesh, args):
    sizes = mesh.shape
    head_dim, (depth, group_cols) = args[8].shape[0], args[4].shape
    nz = sizes["outer"]
    return (
        sizes["inner"] == 2
        and sizes["head"] == 2
        and sizes["clip"] == 2
        and nz == 4
        and args[0].shape[0] == 1
        and args[0].shape[1] % 32 == 0
        and args[7].shape[0] % 64 == 0
        and head_dim % 128 == 0
        and (4 * group_cols) % (2 * nz * head_dim) == 0
        and depth % 32 == 0
    )


def solution(mesh):
    in_specs = (
        P("clip", ("outer", "inner", "head"), None),
        P("clip", None),
        P("clip", None),
        P("clip", None),
        P("outer", ("inner", "head")),
        P("outer", ("inner", "head")),
        P("outer", ("inner", "head")),
        P(("inner", "head"), "outer"),
        P(),
        P(),
    )
    out_specs = P("clip", ("outer", "inner", "head"), None)

    def body(*args):
        if fits(mesh, args):
            return fused(mesh.shape["outer"], *args)
        return per_device(*args)

    return jax.shard_map(
        body, mesh=mesh, in_specs=in_specs, out_specs=out_specs, check_vma=False
    )
```
